32 devices in a mesh: grp: 8 (over z, core), tp: 4 (over y, x).
Axes of the slice: x: 2, y: 2, z: 4, core: 2. Of those that a mesh axis runs over, the one named last changes fastest.
Arguments:
- tokens: bfloat16 [8192, 8192], P('grp'), may hold values from -12 to 12
- joined_weight: bfloat16 [8192, 10240], P(('grp', 'tp')), may hold values from -1.14904852 to 1.14904852
- rollout_lengths: int32 [64], P('grp'), may hold values from 1 to 128
- prompt_of: int32 [64, 1], P('grp'), may hold values from 0 to 7
- score_weight: bfloat16 [8192], P('tp'), may hold values from -0.52734375 to 0.52734375
Outputs:
- attention: bfloat16 [8192, 8192], P('grp', 'tp')
- advantages: float32 [64], P('grp')
The draws below stay inside these ranges and needn't reach their ends.
All inputs are finite; a program needn't handle non-finite values.
Results may differ from the reference program's by a relative error of at most 0.012.
The reference program's roundings to bfloat16 on the way count: a program that leaves them out, or rounds other values in their place, can miss the bound.
Values may be sent and summed in bfloat16 or wider, within the bound.
A program may use at most 128 MiB of HBM per device.

```python
import jax
import jax.numpy as jnp
from jax import lax

MODEL_WIDTH = 8192
QUERY_HEADS = 64
KV_HEAD_COUNT = 8
HEAD_SIZE = 128
ROLL = 8
SLOT = 128
TOK_G = 1024
TOKENS = 8192
ROLLOUTS = 64
PROMPTS = 8
COLS = 10240
N_GRP = 8


def draw_tokens(key, part):
    values = jnp.clip(jax.random.normal(key, (TOKENS, MODEL_WIDTH), jnp.float32), -6.0, 6.0)
    return values.astype(jnp.bfloat16)


def draw_joined_weight(key, part):
    head_ratio = QUERY_HEADS // KV_HEAD_COUNT
    base_offset = jnp.clip(jax.random.normal(key, (MODEL_WIDTH, KV_HEAD_COUNT, head_ratio + 2, HEAD_SIZE), jnp.float32), -6.0, 6.0) * MODEL_WIDTH ** (-0.5)
    return base_offset.reshape(MODEL_WIDTH, COLS).astype(jnp.bfloat16)


def set_ends(entries, own_key, least, top_value):
    longest = entries.shape.index(max(entries.shape))
    spots = []
    for shift in (0, 1):
        where = [jax.random.randint(jax.random.fold_in(own_key, axis), (), 0, length) for axis, length in enumerate(entries.shape)]
        where[longest] = (where[longest] + shift) % entries.shape[longest]
        spots.append(tuple(where))
    return entries.at[spots[0]].set(least).at[spots[1]].set(top_value)


def levels(stream_key, extent, shards, low, high):
    level = 1.0
    for dim, parts in shards:
        steps = jax.random.uniform(jax.random.fold_in(jax.random.fold_in(stream_key, 6), dim), (parts,), jnp.float32, low / len(shards), high / len(shards))
        level = level * jnp.repeat(jnp.exp(steps), extent[dim] // parts).reshape((-1,) + (1,) * (len(extent) - 1 - dim))
    return level


def different_ones(rng, rows, amount, top, lift):
    sequence = jax.random.permutation(jax.random.fold_in(rng, 1), amount)
    boost = sequence
    for power in range(3):
        boost = boost * boost // amount
    boost = boost * lift // amount
    lots = jax.random.randint(jax.random.fold_in(rng, 2), (rows, amount), 0, 4096) + boost
    fixed_rows = jax.random.permutation(jax.random.fold_in(rng, 3), rows)[jnp.arange(amount) % rows]
    lots = jnp.where(jnp.arange(rows)[:, None] == fixed_rows[None, :], 1 << 14, lots)
    priority = lots * amount + jnp.arange(amount)
    return lax.top_k(priority.astype(jnp.int32), top)[1].astype(jnp.int32)


def normal_values(key, dims, deviation, limit, pieces=(), kind=jnp.bfloat16):
    factor_of = levels(key, dims, pieces, -0.22, 0.18) if pieces else 1.0
    result = jax.random.normal(key, dims, jnp.float32) * deviation * factor_of
    return jnp.minimum(jnp.maximum(result, -limit), limit).astype(kind)


def setup_inputs(seed: int = 0) -> dict:
    key_of = jax.random.split(jax.random.key(seed), 6)
    return {
        "tokens": draw_tokens(jax.random.fold_in(key_of[5], 71), 0),
        "joined_weight": draw_joined_weight(jax.random.fold_in(key_of[5], 71), 0),
        "rollout_lengths": set_ends(jax.random.randint(key_of[2], (ROLLOUTS,), 1, SLOT + 1), jax.random.fold_in(key_of[2], 1), 1, SLOT).astype(jnp.int32),
        "prompt_of": different_ones(key_of[3], ROLLOUTS, PROMPTS, 1, 0),
        "score_weight": normal_values(key_of[4], (QUERY_HEADS * HEAD_SIZE,), (8.0 / (QUERY_HEADS * HEAD_SIZE) ** 0.5), 0.52734375, ((0, 4),)),
    }


def attend(joined_matrix, rollout_length_list):
    head_ratio = QUERY_HEADS // KV_HEAD_COUNT
    slot_index = joined_matrix.shape[0] // rollout_length_list.shape[0]
    reshaped_tensor = joined_matrix.reshape(rollout_length_list.shape[0], slot_index, KV_HEAD_COUNT, head_ratio + 2, HEAD_SIZE).astype(jnp.float32)
    queries = reshaped_tensor[:, :, :, :head_ratio, :]
    key_heads = reshaped_tensor[:, :, :, head_ratio, :]
    value_heads = reshaped_tensor[:, :, :, head_ratio + 1, :]
    scores = jnp.einsum('rsgah,rtgh->rgast', queries, key_heads) * HEAD_SIZE ** (-0.5)
    positions = jnp.arange(slot_index)
    allowed = (positions[None, None, :] <= positions[None, :, None]) & (positions[None, None, :] < rollout_length_list[:, None, None])
    scores = jnp.where(allowed[:, None, None], scores, jnp.float32(-1e+30))
    peak = lax.optimization_barrier(jnp.max(scores, axis=-1, keepdims=True))
    expo = jnp.exp(scores - peak)
    probs = (expo / lax.optimization_barrier(jnp.sum(expo, axis=-1, keepdims=True))).astype(jnp.bfloat16)
    mixed = jnp.einsum('rgast,rtgh->rsgah', probs.astype(jnp.float32), value_heads)
    return mixed.reshape(joined_matrix.shape[0], QUERY_HEADS * HEAD_SIZE).astype(jnp.bfloat16)

def reference(tokens, joined_weight, rollout_lengths, prompt_of, score_weight):

    def one_group(items):
        group_tokens, rollout_length_list = items
        joined_matrix = jnp.dot(group_tokens, joined_weight, preferred_element_type=jnp.float32).astype(jnp.bfloat16)
        attention = attend(joined_matrix, rollout_length_list)
        token_score = jnp.dot(attention, score_weight, preferred_element_type=jnp.float32)
        valid = jnp.arange(SLOT)[None, :] < rollout_length_list[:, None]
        reward = lax.optimization_barrier(jnp.sum(jnp.where(valid, token_score.reshape(ROLL, SLOT), jnp.float32(0.0)), axis=1)) / rollout_length_list.astype(jnp.float32)
        return (attention, reward)
    attention, rewards = lax.map(one_group, (tokens.reshape(N_GRP, TOK_G, MODEL_WIDTH), rollout_lengths.reshape(N_GRP, ROLL)))
    attention = attention.reshape(TOKENS, QUERY_HEADS * HEAD_SIZE)
    rewards = rewards.reshape(ROLLOUTS)
    onehot = (prompt_of == jnp.arange(PROMPTS)[None, :]).astype(jnp.float32)
    counts = lax.optimization_barrier(jnp.sum(onehot, axis=0))
    totals = lax.optimization_barrier(jnp.sum(onehot * rewards[:, None], axis=0))
    squares = lax.optimization_barrier(jnp.sum(onehot * (rewards * rewards)[:, None], axis=0))
    divisor = jnp.maximum(counts, 1.0)
    average = totals / divisor
    spread = squares / divisor - average * average
    own_mean = lax.optimization_barrier(jnp.sum(onehot * average[None, :], axis=1))
    own_var = lax.optimization_barrier(jnp.sum(onehot * spread[None, :], axis=1))
    advantages = (rewards - own_mean) / jnp.sqrt(own_var + 0.25)
    return (attention, advantages)
```

```python
import functools

import jax
import jax.numpy as jnp
from jax import lax
from jax.experimental import pallas as pl
from jax.experimental.pallas import tpu as pltpu
from jax.sharding import PartitionSpec as P

QUERY_HEADS = 64
KV_HEAD_COUNT = 8
HEAD_SIZE = 128
CORES = 2
WIDTH = 256
SPLIT = 2


def attend_kernel(groups, chunks, lengths_ref, flag_ref, weight_ref, own, extra, out_ref, reward_ref):
    ratio = QUERY_HEADS // KV_HEAD_COUNT
    per_chunk = own.shape[2] // HEAD_SIZE
    slot = own.shape[1]
    length = lengths_ref[pl.program_id(0)]
    at_end = flag_ref[0] > 0

    def head(index):
        c, h = divmod(index, per_chunk)
        cols = slice(h * HEAD_SIZE, (h + 1) * HEAD_SIZE)
        added = jnp.where(at_end, extra[c, :, cols].astype(jnp.float32), jnp.float32(0.0))
        return (own[c, :, cols] + added).astype(jnp.bfloat16)

    s_pos = lax.broadcasted_iota(jnp.int32, (slot, slot), 0)
    t_pos = lax.broadcasted_iota(jnp.int32, (slot, slot), 1)
    allowed = ((t_pos <= s_pos) & (t_pos < length))[None]
    live = lax.broadcasted_iota(jnp.int32, (slot, HEAD_SIZE), 0) < length
    total = jnp.zeros((slot, HEAD_SIZE), jnp.float32)
    for g in range(groups):
        base = g * (ratio + 2)
        key = head(base + ratio)
        value = head(base + ratio + 1)
        queries = jnp.concatenate([head(base + a) for a in range(ratio)], axis=0)
        scores = lax.dot_general(
            queries, key, (((1,), (1,)), ((), ())), preferred_element_type=jnp.float32
        ) * HEAD_SIZE ** (-0.5)
        scores = jnp.where(allowed, scores.reshape(ratio, slot, slot), jnp.float32(-1e30))
        expo = jnp.exp(scores - jnp.max(scores, axis=-1, keepdims=True))
        probs = expo * (1.0 / jnp.sum(expo, axis=-1, keepdims=True))
        probs = probs.astype(jnp.bfloat16).reshape(ratio * slot, slot)
        mixed = jnp.dot(probs, value, preferred_element_type=jnp.float32).astype(jnp.bfloat16)
        for a in range(ratio):
            part = mixed[a * slot : (a + 1) * slot]
            cols = slice((g * ratio + a) * HEAD_SIZE, (g * ratio + a + 1) * HEAD_SIZE)
            out_ref[:, cols] = part
            total += part.astype(jnp.float32) * weight_ref[:, cols].astype(jnp.float32)
    summed = jnp.sum(jnp.where(live, total, jnp.float32(0.0)), axis=0, keepdims=True)
    summed = jnp.sum(summed, axis=1, keepdims=True)
    reward_ref[...] = jnp.broadcast_to(summed[None], reward_ref.shape)


def attend(own, extra, lengths, flag, score_weight):
    chunks, rows, width = own.shape
    rollouts = lengths.shape[0]
    slot = rows // rollouts
    features = score_weight.shape[0]
    ratio = QUERY_HEADS // KV_HEAD_COUNT
    block = pl.BlockSpec((chunks, slot, width), lambda r, *_: (0, r, 0))
    attention, reward = pl.pallas_call(
        functools.partial(attend_kernel, features // (ratio * HEAD_SIZE), chunks),
        grid_spec=pltpu.PrefetchScalarGridSpec(
            num_scalar_prefetch=2,
            grid=(rollouts,),
            in_specs=[pl.BlockSpec((1, features), lambda r, *_: (0, 0)), block, block],
            out_specs=[
                pl.BlockSpec((slot, features), lambda r, *_: (r, 0)),
                pl.BlockSpec((1, 8, HEAD_SIZE), lambda r, *_: (r, 0, 0)),
            ],
        ),
        out_shape=[
            jax.ShapeDtypeStruct((rows, features), jnp.bfloat16),
            jax.ShapeDtypeStruct((rollouts, 8, HEAD_SIZE), jnp.float32),
        ],
    )(lengths, flag, score_weight.reshape(1, features), own, extra)
    return attention, reward[:, 0, 0]


def project_kernel(
    n, tp_count, tokens, weight, own_out, extra, gath, far,
    tok_v, far_v, w_v, acc, pbuf, send, recv, loads, w_sem, outs, misc,
):
    g = lax.axis_index("grp")
    t = lax.axis_index("tp")
    z, core = g // CORES, g % CORES
    rows, depth = tokens.shape
    chunks, _, width = gath.shape
    own_rows = weight.shape[0]
    half = own_rows * tp_count
    plane = half * CORES
    columns = width * chunks
    part = rows // tp_count
    far_cols = far.shape[1]
    steps = n - 2
    end_steps = n // 2 - 1
    left = z < n // 2
    sign = jnp.where(left, 1, -1)
    is_end = (z == 0) | (z == n - 1)
    inner = (z >= 1) & (z <= n - 2)
    helper = (z == 1) | (z == n - 2)
    first_far = jnp.where(left, 2, 0)
    always = z >= 0
    mid_device = (g + sign * CORES, t)
    end_device = (g - sign * CORES, t)
    sibling = (g + 1 - 2 * core, t)
    end_inner = jnp.where(left, z >= 2, z <= n - 3)
    table = {}
    used = [0]

    def base(key, size):
        if key not in table:
            table[key] = used[0]
            used[0] += size
        return table[key]

    def flow(side, s):
        forth, back = base(("right", s), chunks), base(("left", s), chunks)
        return jnp.where(left, back, forth) if side == "mid" else jnp.where(left, forth, back)

    def local(key):
        return base(key, chunks)

    def remote(i, src, dst, device):
        return pltpu.make_async_remote_copy(
            src_ref=src, dst_ref=dst, send_sem=send.at[i], recv_sem=recv.at[i],
            device_id=device, device_id_type=pl.DeviceIdType.MESH,
        )

    def start(cond, i, src, dst, device):
        @pl.when(cond)
        def _():
            remote(i, src, dst, device).start()

    def arrived(cond, i, dst):
        @pl.when(cond)
        def _():
            remote(i, dst, dst, (g, t)).wait_recv()

    def sent(cond, i, src):
        @pl.when(cond)
        def _():
            remote(i, src, src, (g, t)).wait_send()

    def each(count, body):
        def step(q, carry):
            body(q)
            return carry

        lax.fori_loop(0, count, step, 0)

    def piece(q, who):
        return gath.at[q, pl.ds(pl.multiple_of(z * plane + core * half + who * own_rows, own_rows), own_rows)]

    def block(q, p, c):
        return gath.at[q, pl.ds(pl.multiple_of(p * plane + c * half, half), half)]

    def columns_of(who, q):
        return weight.at[:, pl.ds(pl.multiple_of(who * columns + q * width, width), width)]

    def has(side, s):
        if side == "end":
            return jnp.where(left, z - s >= 0, z + s <= n - 1)
        reach = jnp.where(left, z + s <= n - 1, z - s >= 0)
        return reach if s == 1 else reach & inner

    def plane_of(side, s):
        return jnp.clip(z + sign * s if side == "mid" else z - sign * s, 0, n - 1)

    def own_copy(q):
        return pltpu.make_async_copy(columns_of(t, q), piece(q, t), loads.at[q])

    def scatter(q):
        own_copy(q).start()
        for d in range(1, tp_count):
            start(always, local(("a", d)) + q, columns_of(t ^ d, q), piece(q, t), (g, t ^ d))

    def outward(q, src, dst):
        start(always, flow("end", 1) + q, src, dst, mid_device)
        start(inner, flow("mid", 1) + q, src, dst, end_device)

    def gathered(q, split):
        for d in range(1, tp_count):
            arrived(always, local(("a", d)) + q, piece(q, t ^ d))
            if split:
                outward(q, piece(q, t ^ d), piece(q, t ^ d))
        own_copy(q).wait()
        mine = block(q, z, core)
        if not split:
            outward(q, mine, mine)
        start(always, local("s") + q, mine, mine, sibling)

    def handle(side, s, q):
        here = plane_of(side, s)
        got = block(q, here, core)
        there = has(side, s)
        arrived(there, flow(side, s) + q, got)
        if s < steps:
            if side == "end":
                start(there, flow(side, s + 1) + q, got, got, mid_device)
            else:
                start(there & end_inner, flow(side, s + 1) + q, got, got, end_device)
        start(there, local((side, s)) + q, got, got, sibling)

    def swapped(side, s, q):
        arrived(has(side, s), local((side, s)) + q, block(q, plane_of(side, s), 1 - core))

    def load(slot, q, p):
        return pltpu.make_async_copy(
            gath.at[q, pl.ds(pl.multiple_of(p * plane, plane), plane)], w_v.at[slot], w_sem.at[slot]
        )

    tile = 256

    def over_rows(body):
        each(rows // tile, lambda m: body(pl.ds(pl.multiple_of(m * tile, tile), tile)))

    def columns_at(p):
        return pl.ds(pl.multiple_of(p * plane, plane), plane)

    def gemm(slot, q, p, fresh):
        def body(at):
            product = jnp.dot(tok_v[at, columns_at(p)], w_v[slot], preferred_element_type=jnp.float32)
            if fresh:
                acc[q, at, :] = product
            else:
                acc[q, at, :] += product

        over_rows(body)

    def token_rows(who):
        return far.at[pl.ds(pl.multiple_of(who * part, part), part)]

    def far_source(who):
        return tokens.at[
            pl.ds(pl.multiple_of(who * part, part), part),
            pl.ds(pl.multiple_of(first_far * plane, plane), far_cols),
        ]

    twin = tp_count - 1
    load_tokens = pltpu.make_async_copy(tokens, tok_v, misc.at[0])
    fill = pltpu.make_async_copy(far, far_v, misc.at[1])
    start(is_end, base("t0", 1), far_source(t), token_rows(t), mid_device)
    start(is_end, base("t1", 1), far_source(t ^ twin), token_rows(t ^ twin), mid_device)
    for q in range(SPLIT):
        scatter(q)
        outward(q, columns_of(t, q), piece(q, t))
    each(chunks - SPLIT, lambda q: scatter(q + SPLIT))
    load_tokens.start()
    for q in range(SPLIT):
        gathered(q, True)
    each(chunks - SPLIT, lambda q: gathered(q + SPLIT, False))
    arrived(helper, base("t0", 1), token_rows(t))
    for d in range(1, twin):
        start(helper, base(("g", d), 1), token_rows(t), token_rows(t), (g, t ^ d))
    load_tokens.wait()

    def own_half(q):
        arrived(always, local("s") + q, block(q, z, 1 - core))
        load(q % 2, q, z).start()

    own_half(0)

    def own_step(q):
        @pl.when(q + 1 < chunks)
        def _():
            own_half(q + 1)

        load(q % 2, q, z).wait()
        gemm(q % 2, q, z, True)

    each(chunks, own_step)

    def near_step(q):
        @pl.when(q == chunks - 1)
        def _():
            handle("end", 1, 0)

        handle("mid", 1, q)
        swapped("mid", 1, q)
        p = plane_of("mid", 1)
        load(0, q, p).start()
        load(0, q, p).wait()
        gemm(0, q, p, False)

    each(chunks, near_step)
    arrived(helper, base("t1", 1), token_rows(t ^ twin))
    for d in range(1, twin):
        arrived(helper, base(("g", d), 1), token_rows(t ^ d))

    @pl.when(helper)
    def _():
        fill.start()
        load(0, 0, plane_of("mid", 1)).start()
        fill.wait()

    others = [("mid", s) for s in range(2, steps + 1)] + [("end", s) for s in range(1, end_steps + 1)]
    slot_of = {("mid", 1): 0}
    for other in others:
        slot_of[other] = len(slot_of)

    def product(q):
        return pbuf.at[q % 2]

    def last_step(q):
        @pl.when(q + 1 < chunks)
        def _():
            handle("end", 1, q + 1)

        for s in range(2, steps + 1):
            if s <= end_steps:
                handle("end", s, q)
            handle("mid", s, q)
        for side, s in others:
            swapped(side, s, q)

            @pl.when(has(side, s))
            def _():
                load(slot_of[side, s], q, plane_of(side, s)).start()

        for side, s in others:
            @pl.when(has(side, s))
            def _():
                load(slot_of[side, s], q, plane_of(side, s)).wait()

        @pl.when(helper)
        def _():
            load(0, q, plane_of("mid", 1)).wait()

            @pl.when(q >= 2)
            def _():
                sent(always, local("p") + q - 2, product(q))

            def body(at):
                total = None
                for s in range(1, steps + 1):
                    cols = columns_at(plane_of("mid", s) - first_far)
                    term = jnp.dot(
                        far_v[at, cols], w_v[slot_of["mid", s]], preferred_element_type=jnp.float32
                    )
                    total = term if total is None else total + term
                pbuf[q % 2, at, :] = total.astype(pbuf.dtype)

            over_rows(body)
            remote(local("p") + q, product(q), extra.at[q], end_device).start()

            @pl.when(q + 1 < chunks)
            def _():
                load(0, q + 1, plane_of("mid", 1)).start()

        for side, s in others:
            @pl.when(has(side, s))
            def _():
                gemm(slot_of[side, s], q, plane_of(side, s), False)

        pltpu.make_async_copy(acc.at[q], own_out.at[q], outs.at[q]).start()

    each(chunks, last_step)

    def finish(q):
        arrived(is_end, local("p") + q, extra.at[q])
        pltpu.make_async_copy(acc.at[q], own_out.at[q], outs.at[q]).wait()
        mine = block(q, z, core)
        for d in range(1, tp_count):
            sent(always, local(("a", d)) + q, piece(q, t))
        sent(always, flow("end", 1) + q, mine)
        sent(inner, flow("mid", 1) + q, mine)
        sent(always, local("s") + q, mine)
        for side, count in (("end", end_steps), ("mid", steps)):
            for s in range(1, count + 1):
                there = has(side, s)
                if s < steps:
                    sent(there if side == "end" else there & end_inner, flow(side, s + 1) + q, mine)
                sent(there, local((side, s)) + q, mine)

    each(chunks, finish)
    for q in range(max(chunks - 2, 0), chunks):
        sent(helper, local("p") + q, product(q))
    sent(is_end, base("t0", 1), token_rows(t))
    sent(is_end, base("t1", 1), token_rows(t))
    for d in range(1, twin):
        sent(helper, base(("g", d), 1), token_rows(t))


def project(tokens, weight, n, tp_count):
    rows, depth = tokens.shape
    own_rows = weight.shape[0]
    width = WIDTH
    chunks = weight.shape[1] // tp_count // width
    plane = own_rows * tp_count * CORES
    far = plane * (n - 2)
    steps, end_steps = n - 2, n // 2 - 1
    flows = chunks * (tp_count + 1 + 3 * steps + end_steps) + tp_count
    slots = steps + end_steps
    anywhere = pl.BlockSpec(memory_space=pl.ANY)
    own, extra, *_ = pl.pallas_call(
        functools.partial(project_kernel, n, tp_count),
        in_specs=[anywhere] * 2,
        out_specs=[anywhere] * 4,
        out_shape=[
            jax.ShapeDtypeStruct((chunks, rows, width), jnp.float32),
            jax.ShapeDtypeStruct((chunks, rows, width), jnp.bfloat16),
            jax.ShapeDtypeStruct((chunks, depth, width), jnp.bfloat16),
            jax.ShapeDtypeStruct((rows, far), jnp.bfloat16),
        ],
        scratch_shapes=[
            pltpu.VMEM((rows, depth), jnp.bfloat16),
            pltpu.VMEM((rows, far), jnp.bfloat16),
            pltpu.VMEM((slots, plane, width), jnp.bfloat16),
            pltpu.VMEM((chunks, rows, width), jnp.float32),
            pltpu.VMEM((2, rows, width), jnp.bfloat16),
            pltpu.SemaphoreType.DMA((flows,)),
            pltpu.SemaphoreType.DMA((flows,)),
            pltpu.SemaphoreType.DMA((chunks,)),
            pltpu.SemaphoreType.DMA((slots,)),
            pltpu.SemaphoreType.DMA((chunks,)),
            pltpu.SemaphoreType.DMA((2,)),
        ],
        compiler_params=pltpu.CompilerParams(has_side_effects=True, vmem_limit_bytes=60 * 1024 * 1024),
    )(tokens, weight)
    return own, extra


def share_kernel(grp_count, tp_count, mine, out, held, send, recv, local):
    g = lax.axis_index("grp")
    t = lax.axis_index("tp")

    def copy(i, src, dst, device):
        return pltpu.make_async_remote_copy(
            src_ref=src, dst_ref=dst, send_sem=send.at[i], recv_sem=recv.at[i],
            device_id=device, device_id_type=pl.DeviceIdType.MESH,
        )

    own = pltpu.make_async_copy(mine, held.at[g, t], local)
    own.start()
    first = [copy(d - 1, mine, held.at[g, t], (g, t ^ d)) for d in range(1, tp_count)]
    for c in first:
        c.start()
    own.wait()
    for d in range(1, tp_count):
        copy(d - 1, mine, held.at[g, t ^ d], (g, t)).wait_recv()
    second = [
        copy(tp_count - 1 + d - 1, held.at[g], held.at[g], ((g + d) % grp_count, t))
        for d in range(1, grp_count)
    ]
    for c in second:
        c.start()
    for d in range(1, grp_count):
        source = held.at[(g + grp_count - d) % grp_count]
        copy(tp_count - 1 + d - 1, source, source, (g, t)).wait_recv()
    for c in first + second:
        c.wait_send()
    out[...] = held[...]


def share(mine, grp_count, tp_count):
    shape = (grp_count, tp_count) + mine.shape
    flows = grp_count + tp_count - 2
    return pl.pallas_call(
        functools.partial(share_kernel, grp_count, tp_count),
        in_specs=[pl.BlockSpec(memory_space=pl.ANY)],
        out_specs=pl.BlockSpec(memory_space=pltpu.VMEM),
        out_shape=jax.ShapeDtypeStruct(shape, mine.dtype),
        scratch_shapes=[
            pltpu.VMEM(shape, mine.dtype),
            pltpu.SemaphoreType.DMA((flows,)),
            pltpu.SemaphoreType.DMA((flows,)),
            pltpu.SemaphoreType.DMA,
        ],
        compiler_params=pltpu.CompilerParams(has_side_effects=True),
    )(mine)


def shards(tokens, joined_weight, rollout_lengths, prompt_of, score_weight):
    grp_count = lax.axis_size("grp")
    tp_count = lax.axis_size("tp")
    n = grp_count // CORES
    g = lax.axis_index("grp")
    z = g // CORES
    own, extra = project(tokens, joined_weight, n, tp_count)
    flag = ((z == 0) | (z == n - 1)).astype(jnp.int32).reshape(1)
    attention, reward = attend(own, extra, rollout_lengths, flag, score_weight)
    reward = reward / rollout_lengths.astype(jnp.float32)
    sent = jnp.stack([reward, prompt_of[:, 0].astype(jnp.float32)])
    count = reward.shape[0]
    sent = jnp.pad(sent, ((0, -2 % 8), (0, -count % 128)))
    gathered = share(sent, grp_count, tp_count)[:, :, :2, :count]
    everyone = jnp.sum(gathered[:, :, 0], axis=1).reshape(-1)
    prompts = gathered[:, 0, 1].reshape(-1, 1).astype(jnp.int32)
    labels = jnp.arange(grp_count)[None, :]
    onehot = (prompts == labels).astype(jnp.float32)
    counts = jnp.sum(onehot, axis=0)
    totals = jnp.sum(onehot * everyone[:, None], axis=0)
    squares = jnp.sum(onehot * (everyone * everyone)[:, None], axis=0)
    divisor = jnp.maximum(counts, 1.0)
    average = totals / divisor
    spread = squares / divisor - average * average
    mine = (prompt_of == labels).astype(jnp.float32)
    own_mean = jnp.sum(mine * average[None, :], axis=1)
    own_var = jnp.sum(mine * spread[None, :], axis=1)
    rewards = lax.dynamic_slice(everyone, (g * reward.shape[0],), reward.shape)
    advantages = (rewards - own_mean) / jnp.sqrt(own_var + 0.25)
    return (attention, advantages)


def solution(mesh):
    return jax.shard_map(
        shards,
        mesh=mesh,
        in_specs=(P("grp", None), P(("grp", "tp"), None), P("grp"), P("grp", None), P("tp")),
        out_specs=(P("grp", "tp"), P("grp")),
        check_vma=False,
    )
```

```python
import functools

import jax
import jax.numpy as jnp
from jax import lax
from jax.experimental import pallas as pl
from jax.experimental.pallas import tpu as pltpu
from jax.sharding import PartitionSpec as P

QUERY_HEADS = 64
KV_HEAD_COUNT = 8
HEAD_SIZE = 128
CORES = 2
WIDTH = 256
SPLIT = 2


def fused_kernel(
    n, tp_count, lengths, spans, prompts, score, tokens, weight, attention, advantages, gath, far,
    tok_v, far_v, w_v, acc, pbuf, extra, kv, mixed_v, total, tp_held, grp_held, share_v,
    send, recv, loads, w_sem, outs, misc,
):
    g = lax.axis_index("grp")
    t = lax.axis_index("tp")
    z, core = g // CORES, g % CORES
    rows, depth = tokens.shape
    chunks, _, width = gath.shape
    own_rows = weight.shape[0]
    half = own_rows * tp_count
    plane = half * CORES
    columns = width * chunks
    part = rows // tp_count
    far_cols = far.shape[1]
    steps = n - 2
    end_steps = n // 2 - 1
    left = z < n // 2
    sign = jnp.where(left, 1, -1)
    is_end = (z == 0) | (z == n - 1)
    inner = (z >= 1) & (z <= n - 2)
    helper = (z == 1) | (z == n - 2)
    first_far = jnp.where(left, 2, 0)
    always = z >= 0
    mid_device = (g + sign * CORES, t)
    end_device = (g - sign * CORES, t)
    sibling = (g + 1 - 2 * core, t)
    end_inner = jnp.where(left, z >= 2, z <= n - 3)
    table = {}
    used = [0]

    def base(key, size):
        if key not in table:
            table[key] = used[0]
            used[0] += size
        return table[key]

    def flow(side, s):
        forth, back = base(("right", s), chunks + 1), base(("left", s), chunks + 1)
        return jnp.where(left, back, forth) if side == "mid" else jnp.where(left, forth, back)

    def local(key):
        return base(key, chunks + 1)

    def remote(i, src, dst, device):
        return pltpu.make_async_remote_copy(
            src_ref=src, dst_ref=dst, send_sem=send.at[i], recv_sem=recv.at[i],
            device_id=device, device_id_type=pl.DeviceIdType.MESH,
        )

    def start(cond, i, src, dst, device):
        @pl.when(cond)
        def _():
            remote(i, src, dst, device).start()

    def arrived(cond, i, dst):
        @pl.when(cond)
        def _():
            remote(i, dst, dst, (g, t)).wait_recv()

    def sent(cond, i, src):
        @pl.when(cond)
        def _():
            remote(i, src, src, (g, t)).wait_send()

    def each(count, body):
        def step(q, carry):
            body(q)
            return carry

        lax.fori_loop(0, count, step, 0)

    def piece(q, who):
        return gath.at[q, pl.ds(pl.multiple_of(z * plane + core * half + who * own_rows, own_rows), own_rows)]

    last = chunks - 1
    narrow = width // 2

    def span(h):
        return slice(None) if h is None else slice(h * narrow, (h + 1) * narrow)

    def step_of(q, h):
        return q if h is None else q + h

    def block(q, p, c, h=None):
        return gath.at[q, pl.ds(pl.multiple_of(p * plane + c * half, half), half), span(h)]

    ratio = QUERY_HEADS // KV_HEAD_COUNT
    heads = width // HEAD_SIZE
    per_group = (ratio + 2) // heads

    def columns_of(who, q):
        at = who * columns + (q // per_group * per_group + (q + per_group - 1) % per_group) * width
        return weight.at[:, pl.ds(pl.multiple_of(at, width), width)]

    def has(side, s):
        if side == "end":
            return jnp.where(left, z - s >= 0, z + s <= n - 1)
        reach = jnp.where(left, z + s <= n - 1, z - s >= 0)
        return reach if s == 1 else reach & inner

    def plane_of(side, s):
        return jnp.clip(z + sign * s if side == "mid" else z - sign * s, 0, n - 1)

    def own_copy(q):
        return pltpu.make_async_copy(columns_of(t, q), piece(q, t), loads.at[q])

    def scatter(q):
        own_copy(q).start()
        for d in range(1, tp_count):
            start(always, local(("a", d)) + q, columns_of(t ^ d, q), piece(q, t), (g, t ^ d))

    def outward(q, src, dst):
        start(always, flow("end", 1) + q, src, dst, mid_device)
        start(inner, flow("mid", 1) + q, src, dst, end_device)

    def gathered(q, split):
        for d in range(1, tp_count):
            arrived(always, local(("a", d)) + q, piece(q, t ^ d))
            if split:
                outward(q, piece(q, t ^ d), piece(q, t ^ d))
        own_copy(q).wait()
        mine = block(q, z, core)
        if not split:
            outward(q, mine, mine)
        start(always, local("s") + q, mine, mine, sibling)

    def onward(side, s, q, h):
        got = block(q, plane_of(side, s), core, h)
        at = flow(side, s + 1) + step_of(q, h)
        if side == "end":
            start(has(side, s), at, got, got, mid_device)
        else:
            start(has(side, s) & end_inner, at, got, got, end_device)

    def handle(side, s, q, h=None):
        got = block(q, plane_of(side, s), core, h)
        arrived(has(side, s), flow(side, s) + step_of(q, h), got)
        if s < steps and s == 1:
            @pl.when(q < last)
            def _():
                onward(side, s, q, None)

            @pl.when(q == last)
            def _():
                onward(side, s, last, 0)
                onward(side, s, last, 1)

        elif s < steps:
            onward(side, s, q, h)
        start(has(side, s), local((side, s)) + step_of(q, h), got, got, sibling)

    def swapped(side, s, q, h=None):
        arrived(has(side, s), local((side, s)) + step_of(q, h), block(q, plane_of(side, s), 1 - core, h))

    def load(slot, q, p, h=None):
        return pltpu.make_async_copy(
            gath.at[q, pl.ds(pl.multiple_of(p * plane, plane), plane), span(h)],
            w_v.at[slot, :, span(h)], w_sem.at[slot],
        )

    def columns_at(p):
        return pl.ds(pl.multiple_of(p * plane, plane), plane)

    def gemm(slot, q, p, fresh, h=None):
        result = jnp.dot(tok_v[:, columns_at(p)], w_v[slot, :, span(h)], preferred_element_type=jnp.float32)
        if fresh:
            acc[q] = result
        else:
            acc[q, :, span(h)] += result

    def token_rows(who):
        return far.at[pl.ds(pl.multiple_of(who * part, part), part)]

    def far_source(who):
        return tokens.at[
            pl.ds(pl.multiple_of(who * part, part), part),
            pl.ds(pl.multiple_of(first_far * plane, plane), far_cols),
        ]

    twin = tp_count - 1
    load_tokens = pltpu.make_async_copy(tokens, tok_v, misc.at[0])
    fill = pltpu.make_async_copy(far, far_v, misc.at[1])
    start(is_end, base("t0", 1), far_source(t), token_rows(t), mid_device)
    start(is_end, base("t1", 1), far_source(t ^ twin), token_rows(t ^ twin), mid_device)
    for q in range(SPLIT):
        scatter(q)
        outward(q, columns_of(t, q), piece(q, t))
    each(chunks - SPLIT, lambda q: scatter(q + SPLIT))
    load_tokens.start()
    for q in range(SPLIT):
        gathered(q, True)
    each(chunks - SPLIT, lambda q: gathered(q + SPLIT, False))
    arrived(helper, base("t0", 1), token_rows(t))
    for d in range(1, twin):
        start(helper, base(("g", d), 1), token_rows(t), token_rows(t), (g, t ^ d))
    load_tokens.wait()

    def own_half(q):
        arrived(always, local("s") + q, block(q, z, 1 - core))
        load(q % 2, q, z).start()

    own_half(0)

    def own_step(q):
        @pl.when(q + 1 < chunks)
        def _():
            own_half(q + 1)

        load(q % 2, q, z).wait()
        gemm(q % 2, q, z, True)

    each(chunks, own_step)

    def near_step(q):
        @pl.when(q == chunks - 1)
        def _():
            handle("end", 1, 0)

        handle("mid", 1, q)
        swapped("mid", 1, q)
        p = plane_of("mid", 1)
        load(0, q, p).start()
        load(0, q, p).wait()
        gemm(0, q, p, False)

    each(chunks, near_step)
    if chunks > 1:
        handle("end", 1, 1)
    arrived(helper, base("t1", 1), token_rows(t ^ twin))
    for d in range(1, twin):
        arrived(helper, base(("g", d), 1), token_rows(t ^ d))

    @pl.when(helper)
    def _():
        fill.start()
        load(0, 0, plane_of("mid", 1)).start()
        fill.wait()

    others = [("mid", s) for s in range(2, steps + 1)] + [("end", s) for s in range(1, end_steps + 1)]
    slot_of = {("mid", 1): 0}
    for other in others:
        slot_of[other] = len(slot_of)

    def product(q, h=None):
        return pbuf.at[step_of(q, h) % 2, :, span(h)]

    def retire(q):
        mine = block(q, z, core)
        for d in range(1, tp_count):
            sent(always, local(("a", d)) + q, piece(q, t))
        sent(always, flow("end", 1) + q, mine)
        sent(inner, flow("mid", 1) + q, mine)
        sent(always, local("s") + q, mine)
        for side in ("end", "mid"):
            sent(has(side, 1), local((side, 1)) + q, mine)

    def retire_far(q, h=None):
        mine = block(q, z, core, h)
        at = step_of(q, h)
        for side, count in (("end", end_steps), ("mid", steps)):
            for s in range(1, count + 1):
                if s < steps:
                    there = has(side, s)
                    sent(there if side == "end" else there & end_inner, flow(side, s + 1) + at, mine)
                if s > 1:
                    sent(has(side, s), local((side, s)) + at, mine)

    slot = rows // lengths.shape[0]
    rollouts = lengths.shape[0]
    s_pos = lax.broadcasted_iota(jnp.int32, (slot, slot), 0)
    t_pos = lax.broadcasted_iota(jnp.int32, (slot, slot), 1)

    def rows_of(r):
        return slice(r * slot, (r + 1) * slot)

    def out_index(q):
        return q // per_group * (per_group - 1) + q % per_group - 1

    def out_copy(q, h=None):
        index = out_index(q)
        at = index * width if h is None else index * width + h * narrow
        count = width if h is None else narrow
        cols = pl.ds(pl.multiple_of(at, HEAD_SIZE), count)
        which = index % 2 if h != 1 else 2
        return pltpu.make_async_copy(mixed_v.at[index % 2, :, span(h)], attention.at[:, cols], outs.at[which])

    def attend(q, h=None):
        index = out_index(q)
        if h is None:
            @pl.when(index >= 2)
            def _():
                out_copy(q).wait()

        elif h == 0:
            out_copy(q).wait()
        members = range(heads) if h is None else range(h * heads // 2, (h + 1) * heads // 2)
        weights = score[pl.ds(index, 1), :]
        for r in range(rollouts):
            at = rows_of(r)
            allowed = ((t_pos <= s_pos) & (t_pos < lengths[r]))[None]
            joined = acc[q, at, span(h)].astype(jnp.bfloat16)
            count = len(members)
            queries = jnp.concatenate(
                [joined[:, a * HEAD_SIZE : (a + 1) * HEAD_SIZE] for a in range(count)], axis=0
            )
            scores = lax.dot_general(
                queries, kv[at, :HEAD_SIZE], (((1,), (1,)), ((), ())), preferred_element_type=jnp.float32
            ) * HEAD_SIZE ** (-0.5)
            scores = jnp.where(allowed, scores.reshape(count, slot, slot), jnp.float32(-1e30))
            expo = jnp.exp(scores - jnp.max(scores, axis=-1, keepdims=True))
            probs = expo * (1.0 / jnp.sum(expo, axis=-1, keepdims=True))
            probs = probs.astype(jnp.bfloat16).reshape(count * slot, slot)
            mixed = jnp.dot(probs, kv[at, HEAD_SIZE:], preferred_element_type=jnp.float32).astype(jnp.bfloat16)
            summed = total[at, :]
            for i, a in enumerate(members):
                part_out = mixed[i * slot : (i + 1) * slot]
                cols = slice(a * HEAD_SIZE, (a + 1) * HEAD_SIZE)
                mixed_v[index % 2, at, cols] = part_out
                summed += part_out.astype(jnp.float32) * weights[:, cols]
            total[at, :] = summed
        out_copy(q, h).start()

    total[...] = jnp.zeros_like(total)

    def far_step(q, h=None):
        step = step_of(q, h)
        for s in range(2, steps + 1):
            if s <= end_steps:
                handle("end", s, q, h)
            handle("mid", s, q, h)
        for side, s in others:
            if s > 1 or h != 1:
                swapped(side, s, q, h if s > 1 else None)

            @pl.when(has(side, s))
            def _():
                load(slot_of[side, s], q, plane_of(side, s), h).start()

        for side, s in others:
            @pl.when(has(side, s))
            def _():
                load(slot_of[side, s], q, plane_of(side, s), h).wait()

        @pl.when(helper)
        def _():
            if h != 1:
                load(0, q, plane_of("mid", 1)).wait()

            @pl.when(step >= 2)
            def _():
                sent(always, local("p") + step - 2, pbuf.at[step % 2])

            whole = None
            for s in range(1, steps + 1):
                cols = columns_at(plane_of("mid", s) - first_far)
                term = jnp.dot(
                    far_v[:, cols], w_v[slot_of["mid", s], :, span(h)], preferred_element_type=jnp.float32
                )
                whole = term if whole is None else whole + term
            pbuf[step % 2, :, span(h)] = whole.astype(pbuf.dtype)
            remote(local("p") + step, product(q, h), extra.at[q, :, span(h)], end_device).start()
            if h is None:
                load(0, q + 1, plane_of("mid", 1)).start()

        if h is None:
            @pl.when(q + 2 < chunks)
            def _():
                handle("end", 1, q + 2)

        for side, s in others:
            @pl.when(has(side, s))
            def _():
                gemm(slot_of[side, s], q, plane_of(side, s), False, h)

        arrived(is_end, local("p") + step, extra.at[q, :, span(h)])

        @pl.when(is_end)
        def _():
            acc[q, :, span(h)] += extra[q, :, span(h)].astype(jnp.float32)

        if h is None:
            @pl.when(q % per_group == 0)
            def _():
                kv[...] = acc[q].astype(jnp.bfloat16)

            @pl.when(q % per_group > 0)
            def _():
                attend(q)

            retire(q)

            @pl.when(q >= 1)
            def _():
                retire_far(q - 1)

        else:
            attend(q, h)
            if h == 0:
                retire(q)
                retire_far(q - 1)

    each(last, far_step)
    far_step(last, 0)
    far_step(last, 1)

    lives = []
    for r in range(rollouts):
        live = lax.broadcasted_iota(jnp.int32, (slot, HEAD_SIZE), 0) < lengths[r]
        lives.append(jnp.sum(jnp.where(live, total[rows_of(r), :], jnp.float32(0.0)), axis=0, keepdims=True))
    partial = jnp.sum(jnp.concatenate(lives, axis=0), axis=1, keepdims=True)
    share_v[0] = jnp.broadcast_to(partial, share_v.shape[1:])
    for d in range(1, tp_count):
        start(always, base(("r", d), 1), share_v.at[0], tp_held.at[t], (g, t ^ d))
    tp_held[t] = share_v[0]
    for d in range(1, tp_count):
        arrived(always, base(("r", d), 1), tp_held.at[t ^ d])
    rewards = tp_held[0]
    for who in range(1, tp_count):
        rewards += tp_held[who]
    rewards = rewards / spans[...].astype(jnp.float32)
    lanes = lax.broadcasted_iota(jnp.int32, rewards.shape, 1)
    member = prompts[...] == lanes
    onehot = jnp.where(member, jnp.float32(1.0), jnp.float32(0.0))
    moments = [
        jnp.sum(v, axis=0, keepdims=True) for v in (onehot, onehot * rewards, onehot * (rewards * rewards))
    ]
    filler = jnp.zeros((rewards.shape[0] - 3, rewards.shape[1]), jnp.float32)
    share_v[1] = jnp.concatenate(moments + [filler], axis=0)
    grp_count = n * CORES
    for d in range(1, grp_count):
        start(always, base(("m", d), 1), share_v.at[1], grp_held.at[g], ((g + d) % grp_count, t))
    grp_held[g] = share_v[1]
    for d in range(1, grp_count):
        arrived(always, base(("m", d), 1), grp_held.at[(g + grp_count - d) % grp_count])
    summed = grp_held[0]
    for who in range(1, grp_count):
        summed += grp_held[who]
    divisor = jnp.maximum(summed[0:1], 1.0)
    average = summed[1:2] / divisor
    spread = summed[2:3] / divisor - average * average
    own_mean = jnp.sum(onehot * average, axis=1, keepdims=True)
    own_var = jnp.sum(onehot * spread, axis=1, keepdims=True)
    advantages[...] = (rewards - own_mean) / jnp.sqrt(own_var + 0.25)
    out_copy(last - 1).wait()
    for h in range(2):
        out_copy(last, h).wait()
        retire_far(last, h)
        sent(helper, local("p") + step_of(last, h), product(last, h))
    for d in range(1, tp_count):
        sent(always, base(("r", d), 1), share_v.at[0])
    for d in range(1, grp_count):
        sent(always, base(("m", d), 1), share_v.at[1])
    sent(is_end, base("t0", 1), token_rows(t))
    sent(is_end, base("t1", 1), token_rows(t))
    for d in range(1, twin):
        sent(helper, base(("g", d), 1), token_rows(t))


def fused(tokens, weight, lengths, prompt_of, score_weight, n, tp_count):
    rows, depth = tokens.shape
    own_rows = weight.shape[0]
    width = WIDTH
    chunks = weight.shape[1] // tp_count // width
    plane = own_rows * tp_count * CORES
    far = plane * (n - 2)
    steps, end_steps = n - 2, n // 2 - 1
    features = score_weight.shape[0]
    rollouts = lengths.shape[0]
    flows = (chunks + 1) * (tp_count + 1 + 3 * steps + end_steps) + 2 * tp_count + n * CORES
    slots = steps + end_steps
    anywhere = pl.BlockSpec(memory_space=pl.ANY)
    vmem = pl.BlockSpec(memory_space=pltpu.VMEM)
    attention, advantages, *_ = pl.pallas_call(
        functools.partial(fused_kernel, n, tp_count),
        in_specs=[pl.BlockSpec(memory_space=pltpu.SMEM), vmem, vmem, vmem, anywhere, anywhere],
        out_specs=[anywhere, vmem, anywhere, anywhere],
        out_shape=[
            jax.ShapeDtypeStruct((rows, features), jnp.bfloat16),
            jax.ShapeDtypeStruct((rollouts, HEAD_SIZE), jnp.float32),
            jax.ShapeDtypeStruct((chunks, depth, width), jnp.bfloat16),
            jax.ShapeDtypeStruct((rows, far), jnp.bfloat16),
        ],
        scratch_shapes=[
            pltpu.VMEM((rows, depth), jnp.bfloat16),
            pltpu.VMEM((rows, far), jnp.bfloat16),
            pltpu.VMEM((slots, plane, width), jnp.bfloat16),
            pltpu.VMEM((chunks, rows, width), jnp.float32),
            pltpu.VMEM((2, rows, width), jnp.bfloat16),
            pltpu.VMEM((chunks, rows, width), jnp.bfloat16),
            pltpu.VMEM((rows, 2 * HEAD_SIZE), jnp.bfloat16),
            pltpu.VMEM((2, rows, width), jnp.bfloat16),
            pltpu.VMEM((rows, HEAD_SIZE), jnp.float32),
            pltpu.VMEM((tp_count, rollouts, HEAD_SIZE), jnp.float32),
            pltpu.VMEM((n * CORES, rollouts, HEAD_SIZE), jnp.float32),
            pltpu.VMEM((2, rollouts, HEAD_SIZE), jnp.float32),
            pltpu.SemaphoreType.DMA((flows,)),
            pltpu.SemaphoreType.DMA((flows,)),
            pltpu.SemaphoreType.DMA((chunks,)),
            pltpu.SemaphoreType.DMA((slots,)),
            pltpu.SemaphoreType.DMA((3,)),
            pltpu.SemaphoreType.DMA((2,)),
        ],
        compiler_params=pltpu.CompilerParams(has_side_effects=True, vmem_limit_bytes=62 * 1024 * 1024),
    )(
        lengths, lengths.reshape(rollouts, 1), prompt_of,
        score_weight.reshape(features // width, width).astype(jnp.float32), tokens, weight,
    )
    return attention, advantages[:, 0]


def shards(tokens, joined_weight, rollout_lengths, prompt_of, score_weight):
    n = lax.axis_size("grp") // CORES
    tp_count = lax.axis_size("tp")
    return fused(tokens, joined_weight, rollout_lengths, prompt_of, score_weight, n, tp_count)


def solution(mesh):
    return jax.shard_map(
        shards,
        mesh=mesh,
        in_specs=(P("grp", None), P(("grp", "tp"), None), P("grp"), P("grp", None), P("tp")),
        out_specs=(P("grp", "tp"), P("grp")),
        check_vma=False,
    )
```

```python
import functools

import jax
import jax.numpy as jnp
from jax import lax
from jax.experimental import pallas as pl
from jax.experimental.pallas import tpu as pltpu
from jax.sharding import PartitionSpec as P

QUERY_HEADS = 64
KV_HEAD_COUNT = 8
HEAD_SIZE = 128
CORES = 2
WIDTH = 256
SPLIT = 2


def fused_kernel(
    n, tp_count, lengths, facts, tokens, weight, attention, advantages, gath, far,
    tok_v, far_v, w_v, acc, pbuf, extra, kv, mixed_v, total, tp_held, grp_held, share_v,
    send, recv, loads, w_sem, outs, misc,
):
    g = lax.axis_index("grp")
    t = lax.axis_index("tp")
    z, core = g // CORES, g % CORES
    rows, depth = tokens.shape
    chunks, _, width = gath.shape
    own_rows = weight.shape[0]
    half = own_rows * tp_count
    plane = half * CORES
    columns = width * chunks
    part = rows // tp_count
    far_cols = far.shape[1]
    steps = n - 2
    end_steps = n // 2 - 1
    left = z < n // 2
    sign = jnp.where(left, 1, -1)
    is_end = (z == 0) | (z == n - 1)
    inner = (z >= 1) & (z <= n - 2)
    helper = (z == 1) | (z == n - 2)
    first_far = jnp.where(left, 2, 0)
    always = z >= 0
    mid_device = (g + sign * CORES, t)
    end_device = (g - sign * CORES, t)
    sibling = (g + 1 - 2 * core, t)
    end_inner = jnp.where(left, z >= 2, z <= n - 3)
    table = {}
    used = [0]

    def base(key, size):
        if key not in table:
            table[key] = used[0]
            used[0] += size
        return table[key]

    def flow(side, s):
        forth, back = base(("right", s), chunks + 1), base(("left", s), chunks + 1)
        return jnp.where(left, back, forth) if side == "mid" else jnp.where(left, forth, back)

    def local(key):
        return base(key, chunks + 1)

    def remote(i, src, dst, device):
        return pltpu.make_async_remote_copy(
            src_ref=src, dst_ref=dst, send_sem=send.at[i], recv_sem=recv.at[i],
            device_id=device, device_id_type=pl.DeviceIdType.MESH,
        )

    def start(cond, i, src, dst, device):
        @pl.when(cond)
        def _():
            remote(i, src, dst, device).start()

    def arrived(cond, i, dst):
        @pl.when(cond)
        def _():
            remote(i, dst, dst, (g, t)).wait_recv()

    def sent(cond, i, src):
        @pl.when(cond)
        def _():
            remote(i, src, src, (g, t)).wait_send()

    def each(count, body):
        def step(q, carry):
            body(q)
            return carry

        lax.fori_loop(0, count, step, 0)

    def piece(q, who):
        return gath.at[q, pl.ds(pl.multiple_of(z * plane + core * half + who * own_rows, own_rows), own_rows)]

    last = chunks - 1
    narrow = width // 2

    def span(h):
        return slice(None) if h is None else slice(h * narrow, (h + 1) * narrow)

    def step_of(q, h):
        return q if h is None else q + h

    def block(q, p, c, h=None):
        return gath.at[q, pl.ds(pl.multiple_of(p * plane + c * half, half), half), span(h)]

    ratio = QUERY_HEADS // KV_HEAD_COUNT
    heads = width // HEAD_SIZE
    per_group = (ratio + 2) // heads

    def columns_of(who, q):
        at = who * columns + (q // per_group * per_group + (q + per_group - 1) % per_group) * width
        return weight.at[:, pl.ds(pl.multiple_of(at, width), width)]

    reached = {}
    for s in range(1, n):
        reached["end", s] = jnp.where(left, z - s >= 0, z + s <= n - 1)
        reach = jnp.where(left, z + s <= n - 1, z - s >= 0)
        reached["mid", s] = reach if s == 1 else reach & inner
    passed = {s: reached["mid", s] & end_inner for s in range(1, n)}

    def has(side, s):
        return reached[side, s]

    def plane_of(side, s):
        return jnp.clip(z + sign * s if side == "mid" else z - sign * s, 0, n - 1)

    def own_copy(q):
        return pltpu.make_async_copy(columns_of(t, q), piece(q, t), loads.at[q])

    def scatter(q):
        own_copy(q).start()
        for d in range(1, tp_count):
            start(always, local(("a", d)) + q, columns_of(t ^ d, q), piece(q, t), (g, t ^ d))

    def outward(q, src, dst):
        start(always, flow("end", 1) + q, src, dst, mid_device)
        start(inner, flow("mid", 1) + q, src, dst, end_device)

    def gathered(q, split):
        for d in range(1, tp_count):
            arrived(always, local(("a", d)) + q, piece(q, t ^ d))
            if split:
                outward(q, piece(q, t ^ d), piece(q, t ^ d))
        own_copy(q).wait()
        mine = block(q, z, core)
        if not split:
            outward(q, mine, mine)
        start(always, local("s") + q, mine, mine, sibling)

    def onward(side, s, q, h):
        got = block(q, plane_of(side, s), core, h)
        at = flow(side, s + 1) + step_of(q, h)
        if side == "end":
            start(has(side, s), at, got, got, mid_device)
        else:
            start(passed[s], at, got, got, end_device)

    def handle(side, s, q, h=None):
        got = block(q, plane_of(side, s), core, h)
        arrived(has(side, s), flow(side, s) + step_of(q, h), got)
        if s < steps and s == 1:
            @pl.when(q < last)
            def _():
                onward(side, s, q, None)

            @pl.when(q == last)
            def _():
                onward(side, s, last, 0)
                onward(side, s, last, 1)

        elif s < steps:
            onward(side, s, q, h)
        start(has(side, s), local((side, s)) + step_of(q, h), got, got, sibling)

    def swapped(side, s, q, h=None):
        arrived(has(side, s), local((side, s)) + step_of(q, h), block(q, plane_of(side, s), 1 - core, h))

    def load(slot, q, p, h=None):
        return pltpu.make_async_copy(
            gath.at[q, pl.ds(pl.multiple_of(p * plane, plane), plane), span(h)],
            w_v.at[slot, :, span(h)], w_sem.at[slot],
        )

    def columns_at(p):
        return pl.ds(pl.multiple_of(p * plane, plane), plane)

    def gemm(slot, q, p, fresh, h=None):
        result = jnp.dot(tok_v[:, columns_at(p)], w_v[slot, :, span(h)], preferred_element_type=jnp.float32)
        if fresh:
            acc[q] = result
        else:
            acc[q, :, span(h)] += result

    def token_rows(who):
        return far.at[pl.ds(pl.multiple_of(who * part, part), part)]

    def far_source(who):
        return tokens.at[
            pl.ds(pl.multiple_of(who * part, part), part),
            pl.ds(pl.multiple_of(first_far * plane, plane), far_cols),
        ]

    twin = tp_count - 1
    load_tokens = pltpu.make_async_copy(tokens, tok_v, misc.at[0])
    fill = pltpu.make_async_copy(far, far_v, misc.at[1])
    start(is_end, base("t0", 1), far_source(t), token_rows(t), mid_device)
    start(is_end, base("t1", 1), far_source(t ^ twin), token_rows(t ^ twin), mid_device)
    for q in range(SPLIT):
        scatter(q)
        outward(q, columns_of(t, q), piece(q, t))
    each(chunks - SPLIT, lambda q: scatter(q + SPLIT))
    load_tokens.start()
    for q in range(SPLIT):
        gathered(q, True)
    each(chunks - SPLIT, lambda q: gathered(q + SPLIT, False))
    arrived(helper, base("t0", 1), token_rows(t))
    for d in range(1, twin):
        start(helper, base(("g", d), 1), token_rows(t), token_rows(t), (g, t ^ d))
    load_tokens.wait()

    def own_half(q):
        arrived(always, local("s") + q, block(q, z, 1 - core))
        load(q % 2, q, z).start()

    own_half(0)

    def own_step(q):
        @pl.when(q + 1 < chunks)
        def _():
            own_half(q + 1)

        load(q % 2, q, z).wait()
        gemm(q % 2, q, z, True)

    each(chunks, own_step)

    def near_step(q):
        @pl.when(q == chunks - 1)
        def _():
            handle("end", 1, 0)

        handle("mid", 1, q)
        swapped("mid", 1, q)
        p = plane_of("mid", 1)
        load(0, q, p).start()
        load(0, q, p).wait()
        gemm(0, q, p, False)

    each(chunks, near_step)
    if chunks > 1:
        handle("end", 1, 1)
    arrived(helper, base("t1", 1), token_rows(t ^ twin))
    for d in range(1, twin):
        arrived(helper, base(("g", d), 1), token_rows(t ^ d))

    @pl.when(helper)
    def _():
        fill.start()
        load(0, 0, plane_of("mid", 1)).start()
        fill.wait()

    others = [("mid", s) for s in range(2, steps + 1)] + [("end", s) for s in range(1, end_steps + 1)]
    slot_of = {("mid", 1): 0}
    for other in others:
        slot_of[other] = len(slot_of)

    def product(q, h=None):
        return pbuf.at[step_of(q, h) % 2, :, span(h)]

    def retire(q):
        mine = block(q, z, core)
        for d in range(1, tp_count):
            sent(always, local(("a", d)) + q, piece(q, t))
        sent(always, flow("end", 1) + q, mine)
        sent(inner, flow("mid", 1) + q, mine)
        sent(always, local("s") + q, mine)
        for side in ("end", "mid"):
            sent(has(side, 1), local((side, 1)) + q, mine)

    def retire_far(q, h=None):
        mine = block(q, z, core, h)
        at = step_of(q, h)
        for side, count in (("end", end_steps), ("mid", steps)):
            for s in range(1, count + 1):
                if s < steps:
                    there = has(side, s)
                    sent(there if side == "end" else passed[s], flow(side, s + 1) + at, mine)
                if s > 1:
                    sent(has(side, s), local((side, s)) + at, mine)

    slot = rows // lengths.shape[0]
    rollouts = lengths.shape[0]
    s_pos = lax.broadcasted_iota(jnp.int32, (slot, slot), 0)
    t_pos = lax.broadcasted_iota(jnp.int32, (slot, slot), 1)

    def rows_of(r):
        return slice(r * slot, (r + 1) * slot)

    def out_index(q):
        return q // per_group * (per_group - 1) + q % per_group - 1

    def out_copy(q, h=None):
        index = out_index(q)
        at = index * width if h is None else index * width + h * narrow
        count = width if h is None else narrow
        cols = pl.ds(pl.multiple_of(at, HEAD_SIZE), count)
        which = index % 2 if h != 1 else 2
        return pltpu.make_async_copy(mixed_v.at[index % 2, :, span(h)], attention.at[:, cols], outs.at[which])

    def attend(q, h=None):
        index = out_index(q)
        if h is None:
            @pl.when(index >= 2)
            def _():
                out_copy(q).wait()

        elif h == 0:
            out_copy(q).wait()
        members = range(heads) if h is None else range(h * heads // 2, (h + 1) * heads // 2)
        weights = [facts[pl.ds(index * heads + a, 1), :] for a in members]
        count = len(members)
        every = range(rollouts)
        joined = [acc[q, rows_of(r), span(h)].astype(jnp.bfloat16) for r in every]
        queries = [
            jnp.concatenate([j[:, a * HEAD_SIZE : (a + 1) * HEAD_SIZE] for a in range(count)], axis=0)
            for j in joined
        ]
        scores = [
            lax.dot_general(
                queries[r], kv[rows_of(r), :HEAD_SIZE], (((1,), (1,)), ((), ())),
                preferred_element_type=jnp.float32,
            )
            for r in every
        ]
        mixed = []
        for r in every:
            allowed = ((t_pos <= s_pos) & (t_pos < lengths[r]))[None]
            scaled = (scores[r] * HEAD_SIZE ** (-0.5)).reshape(count, slot, slot)
            scaled = jnp.where(allowed, scaled, jnp.float32(-1e30))
            expo = jnp.exp(scaled - jnp.max(scaled, axis=-1, keepdims=True))
            probs = expo * (1.0 / jnp.sum(expo, axis=-1, keepdims=True))
            probs = probs.astype(jnp.bfloat16).reshape(count * slot, slot)
            mixed.append(jnp.dot(probs, kv[rows_of(r), HEAD_SIZE:], preferred_element_type=jnp.float32))
        for r in every:
            at = rows_of(r)
            rounded = mixed[r].astype(jnp.bfloat16)
            summed = total[at, :]
            for i, a in enumerate(members):
                part_out = rounded[i * slot : (i + 1) * slot]
                mixed_v[index % 2, at, slice(a * HEAD_SIZE, (a + 1) * HEAD_SIZE)] = part_out
                summed += part_out.astype(jnp.float32) * weights[i]
            total[at, :] = summed
        out_copy(q, h).start()

    total[...] = jnp.zeros_like(total)

    def far_handles(q, h=None):
        for s in range(2, steps + 1):
            if s <= end_steps:
                handle("end", s, q, h)
            handle("mid", s, q, h)

    def far_step(q, h=None):
        step = step_of(q, h)
        for side, s in others:
            if s > 1 or h != 1:
                swapped(side, s, q, h if s > 1 else None)

            @pl.when(has(side, s))
            def _():
                load(slot_of[side, s], q, plane_of(side, s), h).start()

        def loaded(chosen):
            for side, s in others:
                if side == chosen:
                    @pl.when(has(side, s))
                    def _():
                        load(slot_of[side, s], q, plane_of(side, s), h).wait()

        loaded("mid")

        @pl.when(helper)
        def _():
            if h != 1:
                load(0, q, plane_of("mid", 1)).wait()

            @pl.when(step >= 2)
            def _():
                sent(always, local("p") + step - 2, pbuf.at[step % 2])

            for part_rows in (slice(0, rows // 2), slice(rows // 2, rows)):
                whole = None
                for s in range(1, steps + 1):
                    cols = columns_at(plane_of("mid", s) - first_far)
                    term = jnp.dot(
                        far_v[part_rows, cols], w_v[slot_of["mid", s], :, span(h)],
                        preferred_element_type=jnp.float32,
                    )
                    whole = term if whole is None else whole + term
                pbuf[step % 2, part_rows, span(h)] = whole.astype(pbuf.dtype)
                remote(
                    local("p") + step, pbuf.at[step % 2, part_rows, span(h)],
                    extra.at[q, part_rows, span(h)], end_device,
                ).start()
            if h is None:
                load(0, q + 1, plane_of("mid", 1)).start()

        if h is None:
            @pl.when(q + 2 < chunks)
            def _():
                handle("end", 1, q + 2)

        loaded("end")
        for side, s in others:
            @pl.when(has(side, s))
            def _():
                gemm(slot_of[side, s], q, plane_of(side, s), False, h)

        if h is None:
            @pl.when(q + 1 < last)
            def _():
                far_handles(q + 1)

            @pl.when(q + 1 == last)
            def _():
                far_handles(last, 0)

        elif h == 0:
            far_handles(last, 1)
        arrived(is_end, local("p") + step, extra.at[q, :, span(h)])

        @pl.when(is_end)
        def _():
            acc[q, :, span(h)] += extra[q, :, span(h)].astype(jnp.float32)

        if h is None:
            @pl.when(q % per_group == 0)
            def _():
                kv[...] = acc[q].astype(jnp.bfloat16)

            @pl.when(q % per_group > 0)
            def _():
                attend(q)

            retire(q)

            @pl.when(q >= 1)
            def _():
                retire_far(q - 1)

        else:
            attend(q, h)
            if h == 0:
                retire(q)
                retire_far(q - 1)

    far_handles(0)
    each(last, far_step)
    far_step(last, 0)
    far_step(last, 1)

    lives = []
    for r in range(rollouts):
        live = lax.broadcasted_iota(jnp.int32, (slot, HEAD_SIZE), 0) < lengths[r]
        lives.append(jnp.sum(jnp.where(live, total[rows_of(r), :], jnp.float32(0.0)), axis=0, keepdims=True))
    partial = jnp.sum(jnp.concatenate(lives, axis=0), axis=1, keepdims=True)
    share_v[0] = jnp.broadcast_to(partial, share_v.shape[1:])
    for d in range(1, tp_count):
        start(always, base(("r", d), 1), share_v.at[0], tp_held.at[t], (g, t ^ d))
    tp_held[t] = share_v[0]
    for d in range(1, tp_count):
        arrived(always, base(("r", d), 1), tp_held.at[t ^ d])
    rewards = tp_held[0]
    for who in range(1, tp_count):
        rewards += tp_held[who]
    features = facts.shape[0] - 2 * rollouts
    rewards = rewards / facts[features : features + rollouts]
    lanes = lax.broadcasted_iota(jnp.int32, rewards.shape, 1)
    member = facts[features + rollouts :] == lanes.astype(jnp.float32)
    onehot = jnp.where(member, jnp.float32(1.0), jnp.float32(0.0))
    moments = [
        jnp.sum(v, axis=0, keepdims=True) for v in (onehot, onehot * rewards, onehot * (rewards * rewards))
    ]
    filler = jnp.zeros((rewards.shape[0] - 3, rewards.shape[1]), jnp.float32)
    share_v[1] = jnp.concatenate(moments + [filler], axis=0)
    grp_count = n * CORES
    for d in range(1, grp_count):
        start(always, base(("m", d), 1), share_v.at[1], grp_held.at[g], ((g + d) % grp_count, t))
    grp_held[g] = share_v[1]
    for d in range(1, grp_count):
        arrived(always, base(("m", d), 1), grp_held.at[(g + grp_count - d) % grp_count])
    summed = grp_held[0]
    for who in range(1, grp_count):
        summed += grp_held[who]
    divisor = jnp.maximum(summed[0:1], 1.0)
    average = summed[1:2] / divisor
    spread = summed[2:3] / divisor - average * average
    own_mean = jnp.sum(onehot * average, axis=1, keepdims=True)
    own_var = jnp.sum(onehot * spread, axis=1, keepdims=True)
    advantages[...] = (rewards - own_mean) / jnp.sqrt(own_var + 0.25)
    out_copy(last - 1).wait()
    for h in range(2):
        out_copy(last, h).wait()
        retire_far(last, h)
        sent(helper, local("p") + step_of(last, h), product(last, h))
    for d in range(1, tp_count):
        sent(always, base(("r", d), 1), share_v.at[0])
    for d in range(1, grp_count):
        sent(always, base(("m", d), 1), share_v.at[1])
    sent(is_end, base("t0", 1), token_rows(t))
    sent(is_end, base("t1", 1), token_rows(t))
    for d in range(1, twin):
        sent(helper, base(("g", d), 1), token_rows(t))


def fused(tokens, weight, lengths, prompt_of, score_weight, n, tp_count):
    rows, depth = tokens.shape
    own_rows = weight.shape[0]
    width = WIDTH
    chunks = weight.shape[1] // tp_count // width
    plane = own_rows * tp_count * CORES
    far = plane * (n - 2)
    steps, end_steps = n - 2, n // 2 - 1
    features = score_weight.shape[0]
    rollouts = lengths.shape[0]
    flows = (chunks + 1) * (tp_count + 1 + 3 * steps + end_steps) + 2 * tp_count + n * CORES
    slots = steps + end_steps
    small = jnp.concatenate([lengths, prompt_of[:, 0]]).astype(jnp.float32)
    table = jnp.concatenate(
        [
            score_weight.reshape(features // HEAD_SIZE, HEAD_SIZE).astype(jnp.float32),
            jnp.broadcast_to(small[:, None], (2 * rollouts, HEAD_SIZE)),
        ]
    )
    anywhere = pl.BlockSpec(memory_space=pl.ANY)
    vmem = pl.BlockSpec(memory_space=pltpu.VMEM)
    attention, advantages, *_ = pl.pallas_call(
        functools.partial(fused_kernel, n, tp_count),
        in_specs=[pl.BlockSpec(memory_space=pltpu.SMEM), vmem, anywhere, anywhere],
        out_specs=[anywhere, vmem, anywhere, anywhere],
        out_shape=[
            jax.ShapeDtypeStruct((rows, features), jnp.bfloat16),
            jax.ShapeDtypeStruct((rollouts, HEAD_SIZE), jnp.float32),
            jax.ShapeDtypeStruct((chunks, depth, width), jnp.bfloat16),
            jax.ShapeDtypeStruct((rows, far), jnp.bfloat16),
        ],
        scratch_shapes=[
            pltpu.VMEM((rows, depth), jnp.bfloat16),
            pltpu.VMEM((rows, far), jnp.bfloat16),
            pltpu.VMEM((slots, plane, width), jnp.bfloat16),
            pltpu.VMEM((chunks, rows, width), jnp.float32),
            pltpu.VMEM((2, rows, width), jnp.bfloat16),
            pltpu.VMEM((chunks, rows, width), jnp.bfloat16),
            pltpu.VMEM((rows, 2 * HEAD_SIZE), jnp.bfloat16),
            pltpu.VMEM((2, rows, width), jnp.bfloat16),
            pltpu.VMEM((rows, HEAD_SIZE), jnp.float32),
            pltpu.VMEM((tp_count, rollouts, HEAD_SIZE), jnp.float32),
            pltpu.VMEM((n * CORES, rollouts, HEAD_SIZE), jnp.float32),
            pltpu.VMEM((2, rollouts, HEAD_SIZE), jnp.float32),
            pltpu.SemaphoreType.DMA((flows,)),
            pltpu.SemaphoreType.DMA((flows,)),
            pltpu.SemaphoreType.DMA((chunks,)),
            pltpu.SemaphoreType.DMA((slots,)),
            pltpu.SemaphoreType.DMA((3,)),
            pltpu.SemaphoreType.DMA((2,)),
        ],
        compiler_params=pltpu.CompilerParams(has_side_effects=True, vmem_limit_bytes=62 * 1024 * 1024),
    )(lengths, table, tokens, weight)
    return attention, advantages[:, 0]


def shards(tokens, joined_weight, rollout_lengths, prompt_of, score_weight):
    n = lax.axis_size("grp") // CORES
    tp_count = lax.axis_size("tp")
    return fused(tokens, joined_weight, rollout_lengths, prompt_of, score_weight, n, tp_count)


def solution(mesh):
    return jax.shard_map(
        shards,
        mesh=mesh,
        in_specs=(P("grp", None), P(("grp", "tp"), None), P("grp"), P("grp", None), P("tp")),
        out_specs=(P("grp", "tp"), P("grp")),
        check_vma=False,
    )
```
